1024 devices in a mesh: segment: 16 (over z_hi, x), dp: 8 (over z_lo, core), tensor: 8 (over y).
Axes of the slice: x: 8, y: 8, z: 8 (z_hi: 2, z_lo: 4; z = z_hi * 4 + z_lo), core: 2. Of those that a mesh axis runs over, the one named last changes fastest.
Arguments:
- acts: bfloat16 [16, 2048, 1024], P('segment', ('dp', 'tensor')), may hold values from -6 to 6
- norm_gain: float32 [16, 1024], P('segment'), may hold values from 0.1 to 1.9
- final_gain: float32 [1024], replicated, may hold values from 0.1 to 1.9
- w_query: bfloat16 [16, 1024, 8192], P('segment', None, 'tensor'), may hold values from -0.015625 to 0.015625
- w_key: bfloat16 [16, 1024, 8192], P('segment', None, 'tensor'), may hold values from -0.1875 to 0.1875
- w_value: bfloat16 [16, 1024, 8192], P('segment', None, 'tensor'), may hold values from -0.1875 to 0.1875
- w_out: bfloat16 [16, 8192, 1024], P('segment', 'tensor'), may hold values from -0.0625 to 0.0625
- cache: bfloat16 [16, 2, 2048, 8192], P('segment', None, 'dp', 'tensor'), may hold values from -6 to 6
Outputs:
- updated: bfloat16 [16, 2048, 1024], P('segment', ('dp', 'tensor'))
- fresh: bfloat16 [16, 2, 2048, 8192], P('segment', None, 'dp', 'tensor')
The draws below stay inside these ranges and needn't reach their ends.
All inputs are finite; a program needn't handle non-finite values.
Results may differ from the reference program's by a relative error of at most 0.01.
Values may be sent and summed in bfloat16 or wider, within the bound.
No kernel may reach another device: no remote copies, remote signals or barrier semaphores. Data moves between devices by JAX's collectives and lax.ppermute only.
A program may use at most 64 MiB of HBM per device.

```python
import jax
import jax.numpy as jnp
from jax import lax

D = 1024
HDIM = 128
INNER = 8192
LEN = 256
ROWS = 2048
ENC = 8
N_SEGMENT = 16
N_DP = 8
N_TENSOR = 8


def levels(stream_key, shape, shards, smallest, largest):
    factor_of = 1.0
    for position, shards_of in shards:
        draws = jax.random.uniform(jax.random.fold_in(jax.random.fold_in(stream_key, 6), position), (shards_of,), jnp.float32, smallest / len(shards), largest / len(shards))
        factor_of = factor_of * jnp.repeat(jnp.exp(draws), shape[position] // shards_of).reshape((-1,) + (1,) * (len(shape) - 1 - position))
    return factor_of


def scatter_about(key, shape, scale, limit, shards=(), dtype=jnp.bfloat16):
    level = levels(key, shape, shards, -0.22, 0.18) if shards else 1.0
    entries = jax.random.normal(key, shape, jnp.float32) * scale * level
    return jnp.minimum(jnp.maximum(entries, -limit), limit).astype(dtype)


def setup_inputs(seed: int = 0) -> dict:
    arg_keys = jax.random.split(jax.random.key(seed), 9)
    acts = scatter_about(arg_keys[0], (N_SEGMENT, ROWS, D), 1.0, 6.0, ((0, 16), (1, 64)))
    norm_gain = jnp.clip(1.0 + 0.18 * jax.random.normal(arg_keys[1], (N_SEGMENT, D), jnp.float32), 0.1, 1.9)
    final_gain = jnp.clip(1.0 + 0.18 * jax.random.normal(arg_keys[2], (D,), jnp.float32), 0.1, 1.9)
    w_query = scatter_about(arg_keys[3], (N_SEGMENT, D, INNER), (D * HDIM) ** -0.5, 0.015625, ((0, 16), (2, 8)))
    w_key = scatter_about(arg_keys[4], (N_SEGMENT, D, INNER), D ** -0.5, 0.1875, ((0, 16), (2, 8)))
    w_value = scatter_about(arg_keys[5], (N_SEGMENT, D, INNER), D ** -0.5, 0.1875, ((0, 16), (2, 8)))
    w_out = scatter_about(arg_keys[6], (N_SEGMENT, INNER, D), INNER ** -0.5, 0.0625, ((0, 16), (1, 8)))
    cache = scatter_about(arg_keys[7], (N_SEGMENT, 2, ROWS, INNER), 1.0, 6.0, ((0, 16), (2, 8), (3, 8)))
    return dict(acts=acts, norm_gain=norm_gain, final_gain=final_gain, w_query=w_query, w_key=w_key, w_value=w_value, w_out=w_out, cache=cache)


EPSILON = 1e-06

def normalize(values, gain):
    wide = values.astype(jnp.float32)
    scale = lax.rsqrt(lax.optimization_barrier(jnp.mean(wide * wide, axis=-1, keepdims=True)) + EPSILON)
    return (wide * scale * gain.astype(jnp.float32)).astype(jnp.bfloat16)

def attend(queries, keys, values):
    length = queries.shape[0]
    heads = queries.shape[1] // HDIM
    query_heads = queries.reshape(length, heads, HDIM).astype(jnp.float32)
    key_heads = keys.reshape(keys.shape[0], heads, HDIM).astype(jnp.float32)
    value_heads = values.reshape(values.shape[0], heads, HDIM).astype(jnp.float32)
    scores = jnp.einsum('qhd,khd->hqk', query_heads, key_heads)
    weights = jnp.exp(scores)
    probs = (weights / lax.optimization_barrier(jnp.sum(weights, axis=-1, keepdims=True))).astype(jnp.bfloat16)
    context = jnp.einsum('hqk,khd->qhd', probs.astype(jnp.float32), value_heads)
    return context.reshape(length, heads * HDIM).astype(jnp.bfloat16)

def section(tokens, gain, w_query, w_key, w_value, w_out, cache, memory, decoder):
    normed = normalize(tokens, gain)
    queries = jnp.dot(normed, w_query, preferred_element_type=jnp.float32).astype(jnp.bfloat16)
    own_keys = jnp.dot(normed, w_key, preferred_element_type=jnp.float32).astype(jnp.bfloat16)
    own_values = jnp.dot(normed, w_value, preferred_element_type=jnp.float32).astype(jnp.bfloat16)
    keys = jnp.where(decoder, cache[0], own_keys)
    values = jnp.where(decoder, cache[1], own_values)
    inner = queries.shape[1]
    trio = (queries.reshape(N_DP, LEN, inner), keys.reshape(N_DP, LEN, inner), values.reshape(N_DP, LEN, inner))
    context = lax.map(lambda item: attend(item[0], item[1], item[2]), trio).reshape(ROWS, inner)
    group = inner // N_TENSOR
    context_groups = jnp.transpose(context.reshape(ROWS, N_TENSOR, group), (1, 0, 2))
    weight_groups = w_out.reshape(N_TENSOR, group, D)

    def group_term(pair):
        rounded = jnp.dot(pair[0], pair[1], preferred_element_type=jnp.float32).astype(jnp.bfloat16)
        rounded = lax.optimization_barrier(rounded)
        return rounded.astype(jnp.float32)
    partials = lax.map(group_term, (context_groups, weight_groups))
    branch = lax.optimization_barrier(jnp.sum(partials, axis=0))
    updated = (tokens.astype(jnp.float32) + branch).astype(jnp.bfloat16)
    memory_keys = jnp.dot(memory, w_key, preferred_element_type=jnp.float32).astype(jnp.bfloat16)
    memory_values = jnp.dot(memory, w_value, preferred_element_type=jnp.float32).astype(jnp.bfloat16)
    fresh = jnp.where(decoder, jnp.stack([memory_keys, memory_values]), jnp.stack([own_keys, own_values]))
    return (updated, fresh)

def reference(acts, norm_gain, final_gain, w_query, w_key, w_value, w_out, cache):
    root = ENC - 1
    blank = jnp.zeros((ROWS, D), jnp.bfloat16)
    root_updated, unused = section(acts[root], norm_gain[root], w_query[root], w_key[root], w_value[root], w_out[root], cache[root], blank, False)
    memory = normalize(root_updated, final_gain)
    indices = jnp.arange(N_SEGMENT).astype(jnp.int32)

    def one_section(item):
        return section(item[0], item[1], item[2], item[3], item[4], item[5], item[6], memory, item[7] >= ENC)
    updated, fresh = lax.map(one_section, (acts, norm_gain, w_query, w_key, w_value, w_out, cache, indices))
    return (updated, fresh)
```

```python
import jax
import jax.numpy as jnp
from jax import lax
from jax.experimental import pallas as pl
from jax.experimental.pallas import tpu as pltpu
from jax.sharding import PartitionSpec as P

HDIM = 128


EPSILON = 1e-06

SEND_ORDER = (3, 2, 4, 1, 5, 0, 6, 7)


def gathered_copies(x, axis):
    devices = lax.axis_size(axis)
    copies = jnp.broadcast_to(x[None], (devices, *x.shape))
    return lax.all_to_all(copies, axis, 0, 0, tiled=True)


def dot(a, b):
    return jnp.dot(a, b, preferred_element_type=jnp.float32)


def normalize(wide, gain):
    scale = lax.rsqrt(jnp.mean(wide * wide, axis=-1, keepdims=True) + EPSILON)
    return (wide * scale * gain).astype(jnp.bfloat16)


def is_decoder():
    return lax.axis_index("segment") >= lax.axis_size("segment") // 2


def attention_kernel(rows, gain_far, w_query, w_key, w_value, w_out, cache, partial, made, gain, kv, wq, wk, wv, wo, queries, context, sems):
    decoder = is_decoder()
    gain_copy = pltpu.make_async_copy(gain_far, gain, sems.at[0])
    key_copy = pltpu.make_async_copy(w_key, wk, sems.at[1])
    value_copy = pltpu.make_async_copy(w_value, wv, sems.at[2])
    out_copy = pltpu.make_async_copy(w_out, wo, sems.at[3])
    cache_copy = pltpu.make_async_copy(cache, kv, sems.at[4])
    made_copy = pltpu.make_async_copy(kv, made, sems.at[5])
    query_copies = []
    for part in range(2):
        cols = slice(part * wq.shape[1] // 2, (part + 1) * wq.shape[1] // 2)
        query_copies.append((cols, pltpu.make_async_copy(w_query.at[:, cols], wq.at[:, cols], sems.at[6 + part])))
    gain_copy.start()
    for _, copy in query_copies:
        copy.start()

    @pl.when(decoder)
    def _():
        cache_copy.start()

    @pl.when(jnp.logical_not(decoder))
    def _():
        key_copy.start()
        value_copy.start()

    out_copy.start()
    gain_copy.wait()
    normed = normalize(rows[...].astype(jnp.float32), gain[...])
    for cols, copy in query_copies:
        copy.wait()
        queries[:, cols] = dot(normed, wq[:, cols]).astype(jnp.bfloat16)

    @pl.when(decoder)
    def _():
        cache_copy.wait()

    @pl.when(jnp.logical_not(decoder))
    def _():
        key_copy.wait()
        kv[0] = dot(normed, wk[...]).astype(jnp.bfloat16)
        value_copy.wait()
        kv[1] = dot(normed, wv[...]).astype(jnp.bfloat16)
        made_copy.start()

    for head in range(queries.shape[1] // HDIM):
        cols = slice(head * HDIM, (head + 1) * HDIM)
        scores = lax.dot_general(queries[:, cols], kv[0, :, cols], (((1,), (1,)), ((), ())), preferred_element_type=jnp.float32)
        weights = jnp.exp(scores - jnp.max(scores, axis=-1, keepdims=True))
        inverse = 1.0 / jnp.sum(weights, axis=-1, keepdims=True)
        probs = (weights * inverse).astype(jnp.bfloat16)
        context[:, cols] = dot(probs, kv[1, :, cols]).astype(jnp.bfloat16)
    out_copy.wait()
    partial[...] = dot(context[...], wo[...]).astype(jnp.bfloat16)

    @pl.when(jnp.logical_not(decoder))
    def _():
        made_copy.wait()


NEAR = pl.BlockSpec(memory_space=pltpu.VMEM)
FAR = pl.BlockSpec(memory_space=pltpu.HBM)
PARAMS = pltpu.CompilerParams(vmem_limit_bytes=40 << 20)


def far(*arrays):
    return [pltpu.with_memory_space_constraint(x, pltpu.HBM) for x in arrays]


def attention(rows, gain, w_query, w_key, w_value, w_out, cache):
    weights = far(gain, w_query, w_key, w_value, w_out, cache)
    length, width = rows.shape
    bf16 = jnp.bfloat16
    inner = w_query.shape[1]
    return pl.pallas_call(
        attention_kernel,
        out_shape=(jax.ShapeDtypeStruct((length, width), bf16), jax.ShapeDtypeStruct((2, length, inner), bf16)),
        in_specs=[NEAR, FAR, FAR, FAR, FAR, FAR, FAR],
        out_specs=(NEAR, FAR),
        scratch_shapes=[
            pltpu.VMEM(gain.shape, jnp.float32),
            pltpu.VMEM((2, length, inner), bf16),
            pltpu.VMEM(w_query.shape, bf16),
            pltpu.VMEM(w_key.shape, bf16),
            pltpu.VMEM(w_value.shape, bf16),
            pltpu.VMEM(w_out.shape, bf16),
            pltpu.VMEM((length, inner), bf16),
            pltpu.VMEM((length, inner), bf16),
            pltpu.SemaphoreType.DMA((8,)),
        ],
        compiler_params=PARAMS,
        name="section_attention",
    )(rows, *weights)


def residual_kernel(arrived, tokens, gain, updated, memory):
    branch = jnp.sum(arrived[...].astype(jnp.float32), axis=0)
    new = (tokens[...].astype(jnp.float32) + branch).astype(jnp.bfloat16)
    updated[...] = new
    memory[...] = normalize(new.astype(jnp.float32), gain[...])


def residual(arrived, tokens, gain):
    shape = jax.ShapeDtypeStruct(tokens.shape, tokens.dtype)
    return pl.pallas_call(
        residual_kernel,
        out_shape=(shape, shape),
        in_specs=[NEAR, NEAR, NEAR],
        out_specs=(NEAR, NEAR),
        compiler_params=PARAMS,
        name="residual_norm",
    )(arrived, tokens, gain)


def memory_kernel(memory, new, w_key, w_value, made, updated, fresh, wv, kv, sems):
    del made
    decoder = is_decoder()
    new_copy = pltpu.make_async_copy(new, updated, sems.at[5])
    new_copy.start()
    weight_copy = pltpu.make_async_copy(w_value, wv, sems.at[0])
    pieces = []
    for which in range(2):
        for part in range(2):
            span = (which, slice(part * kv.shape[1] // 2, (part + 1) * kv.shape[1] // 2))
            pieces.append((span, pltpu.make_async_copy(kv.at[span], fresh.at[span], sems.at[1 + len(pieces)])))

    @pl.when(decoder)
    def _():
        weight_copy.start()
        for span, copy in pieces:
            if span[0] == 1 and span[1].start == 0:
                weight_copy.wait()
            kv[span] = dot(memory[span[1], :], (wv if span[0] else w_key)[...]).astype(jnp.bfloat16)
            copy.start()
        for _, copy in pieces:
            copy.wait()

    new_copy.wait()


def memory_pair(memory, new, w_key, w_value, made):
    (w_value,) = far(w_value)
    return pl.pallas_call(
        memory_kernel,
        out_shape=(jax.ShapeDtypeStruct(new.shape, new.dtype), jax.ShapeDtypeStruct(made.shape, made.dtype)),
        in_specs=[NEAR, NEAR, NEAR, FAR, FAR],
        out_specs=(FAR, FAR),
        scratch_shapes=[
            pltpu.VMEM(w_value.shape, w_value.dtype),
            pltpu.VMEM(made.shape, made.dtype),
            pltpu.SemaphoreType.DMA((6,)),
        ],
        input_output_aliases={4: 1},
        compiler_params=PARAMS,
        name="memory_pair",
    )(memory, new, w_key, w_value, made)


def on_device(acts, norm_gain, final_gain, w_query, w_key, w_value, w_out, cache):
    tokens = acts[0]
    rows, width = tokens.shape
    tensor = lax.axis_size("tensor")
    half = lax.axis_size("segment") // 2
    all_rows = gathered_copies(tokens, "tensor").reshape(tensor * rows, width)
    partial, made = attention(all_rows, norm_gain, w_query[0], w_key[0], w_value[0], w_out[0], cache[0])
    arrived = lax.all_to_all(partial.reshape(tensor, rows, width), "tensor", 0, 0, tiled=True)
    new, memory_part = residual(arrived, tokens, final_gain[None])
    holding = [lax.ppermute(memory_part, "segment", [(half - 1, half + to)]) for to in SEND_ORDER]
    segment = lax.axis_index("segment")
    mine = holding[0]
    for to, sent in zip(SEND_ORDER[1:], holding[1:]):
        mine = jnp.where(segment == half + to, sent, mine)
    memory = gathered_copies(mine, "tensor").reshape(tensor * rows, width)
    updated, fresh = memory_pair(memory, new, w_key[0], w_value[0], made)
    return (updated[None], fresh[None])


def solution(mesh):
    placed = (
        P("segment", ("dp", "tensor"), None),
        P("segment", None),
        P(),
        P("segment", None, "tensor"),
        P("segment", None, "tensor"),
        P("segment", None, "tensor"),
        P("segment", "tensor", None),
        P("segment", None, "dp", "tensor"),
    )
    return jax.shard_map(
        on_device,
        mesh=mesh,
        in_specs=placed,
        out_specs=(P("segment", ("dp", "tensor"), None), P("segment", None, "dp", "tensor")),
        check_vma=False,
    )
```

```python
import jax
import jax.numpy as jnp
from jax import lax
from jax.experimental import pallas as pl
from jax.experimental.pallas import tpu as pltpu
from jax.sharding import PartitionSpec as P

HDIM = 128


EPSILON = 1e-06

FIRST = (1, 5, 3, 0, 6, 7)
SECOND = ((1, 2), (5, 4))


def gathered_copies(x, axis):
    devices = lax.axis_size(axis)
    copies = jnp.broadcast_to(x[None], (devices, *x.shape))
    return lax.all_to_all(copies, axis, 0, 0, tiled=True)


def dot(a, b):
    return jnp.dot(a, b, preferred_element_type=jnp.float32)


def normalize(wide, gain):
    scale = lax.rsqrt(jnp.mean(wide * wide, axis=-1, keepdims=True) + EPSILON)
    return (wide * scale * gain).astype(jnp.bfloat16)


def is_decoder():
    return lax.axis_index("segment") >= lax.axis_size("segment") // 2


def attention_kernel(rows, gain_far, w_query, w_key, w_value, w_out, cache, partial, made, gain, kv, wq, wk, wv, wo, queries, context, sems):
    decoder = is_decoder()
    gain_copy = pltpu.make_async_copy(gain_far, gain, sems.at[0])
    key_copy = pltpu.make_async_copy(w_key, wk, sems.at[1])
    value_copy = pltpu.make_async_copy(w_value, wv, sems.at[2])
    out_copy = pltpu.make_async_copy(w_out, wo, sems.at[3])
    cache_copy = pltpu.make_async_copy(cache, kv, sems.at[4])
    made_copy = pltpu.make_async_copy(kv, made, sems.at[5])
    query_copies = []
    for part in range(2):
        cols = slice(part * wq.shape[1] // 2, (part + 1) * wq.shape[1] // 2)
        query_copies.append((cols, pltpu.make_async_copy(w_query.at[:, cols], wq.at[:, cols], sems.at[6 + part])))
    gain_copy.start()
    for _, copy in query_copies:
        copy.start()

    @pl.when(decoder)
    def _():
        cache_copy.start()

    @pl.when(jnp.logical_not(decoder))
    def _():
        key_copy.start()
        value_copy.start()

    out_copy.start()
    gain_copy.wait()
    normed = normalize(rows[...].astype(jnp.float32), gain[...])
    for cols, copy in query_copies:
        copy.wait()
        queries[:, cols] = dot(normed, wq[:, cols]).astype(jnp.bfloat16)

    @pl.when(decoder)
    def _():
        cache_copy.wait()

    @pl.when(jnp.logical_not(decoder))
    def _():
        key_copy.wait()
        kv[0] = dot(normed, wk[...]).astype(jnp.bfloat16)
        value_copy.wait()
        kv[1] = dot(normed, wv[...]).astype(jnp.bfloat16)
        made_copy.start()

    for head in range(queries.shape[1] // HDIM):
        cols = slice(head * HDIM, (head + 1) * HDIM)
        scores = lax.dot_general(queries[:, cols], kv[0, :, cols], (((1,), (1,)), ((), ())), preferred_element_type=jnp.float32)
        weights = jnp.exp(scores - jnp.max(scores, axis=-1, keepdims=True))
        inverse = 1.0 / jnp.sum(weights, axis=-1, keepdims=True)
        probs = (weights * inverse).astype(jnp.bfloat16)
        context[:, cols] = dot(probs, kv[1, :, cols]).astype(jnp.bfloat16)
    out_copy.wait()
    partial[...] = dot(context[...], wo[...]).astype(jnp.bfloat16)

    @pl.when(jnp.logical_not(decoder))
    def _():
        made_copy.wait()


NEAR = pl.BlockSpec(memory_space=pltpu.VMEM)
FAR = pl.BlockSpec(memory_space=pltpu.HBM)
PARAMS = pltpu.CompilerParams(vmem_limit_bytes=40 << 20)


def far(*arrays):
    return [pltpu.with_memory_space_constraint(x, pltpu.HBM) for x in arrays]


def attention(rows, gain, w_query, w_key, w_value, w_out, cache):
    weights = far(gain, w_query, w_key, w_value, w_out, cache)
    length, width = rows.shape
    bf16 = jnp.bfloat16
    inner = w_query.shape[1]
    return pl.pallas_call(
        attention_kernel,
        out_shape=(jax.ShapeDtypeStruct((length, width), bf16), jax.ShapeDtypeStruct((2, length, inner), bf16)),
        in_specs=[NEAR, FAR, FAR, FAR, FAR, FAR, FAR],
        out_specs=(NEAR, FAR),
        scratch_shapes=[
            pltpu.VMEM(gain.shape, jnp.float32),
            pltpu.VMEM((2, length, inner), bf16),
            pltpu.VMEM(w_query.shape, bf16),
            pltpu.VMEM(w_key.shape, bf16),
            pltpu.VMEM(w_value.shape, bf16),
            pltpu.VMEM(w_out.shape, bf16),
            pltpu.VMEM((length, inner), bf16),
            pltpu.VMEM((length, inner), bf16),
            pltpu.SemaphoreType.DMA((8,)),
        ],
        compiler_params=PARAMS,
        name="section_attention",
    )(rows, *weights)


def residual_kernel(arrived, tokens, gain, updated, memory):
    branch = jnp.sum(arrived[...].astype(jnp.float32), axis=0)
    new = (tokens[...].astype(jnp.float32) + branch).astype(jnp.bfloat16)
    updated[...] = new
    memory[...] = normalize(new.astype(jnp.float32), gain[...])


def residual(arrived, tokens, gain):
    shape = jax.ShapeDtypeStruct(tokens.shape, tokens.dtype)
    return pl.pallas_call(
        residual_kernel,
        out_shape=(shape, shape),
        in_specs=[NEAR, NEAR, NEAR],
        out_specs=(NEAR, NEAR),
        compiler_params=PARAMS,
        name="residual_norm",
    )(arrived, tokens, gain)


def memory_kernel(memory, new, w_key, w_value, made, updated, fresh, wv, kv, sems):
    del made
    decoder = is_decoder()
    new_copy = pltpu.make_async_copy(new, updated, sems.at[5])
    new_copy.start()
    weight_copy = pltpu.make_async_copy(w_value, wv, sems.at[0])
    pieces = []
    for which in range(2):
        for part in range(2):
            span = (which, slice(part * kv.shape[1] // 2, (part + 1) * kv.shape[1] // 2))
            pieces.append((span, pltpu.make_async_copy(kv.at[span], fresh.at[span], sems.at[1 + len(pieces)])))

    @pl.when(decoder)
    def _():
        weight_copy.start()
        for span, copy in pieces:
            if span[0] == 1 and span[1].start == 0:
                weight_copy.wait()
            kv[span] = dot(memory[span[1], :], (wv if span[0] else w_key)[...]).astype(jnp.bfloat16)
            copy.start()
        for _, copy in pieces:
            copy.wait()

    new_copy.wait()


def memory_pair(memory, new, w_key, w_value, made):
    (w_value,) = far(w_value)
    return pl.pallas_call(
        memory_kernel,
        out_shape=(jax.ShapeDtypeStruct(new.shape, new.dtype), jax.ShapeDtypeStruct(made.shape, made.dtype)),
        in_specs=[NEAR, NEAR, NEAR, FAR, FAR],
        out_specs=(FAR, FAR),
        scratch_shapes=[
            pltpu.VMEM(w_value.shape, w_value.dtype),
            pltpu.VMEM(made.shape, made.dtype),
            pltpu.SemaphoreType.DMA((6,)),
        ],
        input_output_aliases={4: 1},
        compiler_params=PARAMS,
        name="memory_pair",
    )(memory, new, w_key, w_value, made)


def on_device(acts, norm_gain, final_gain, w_query, w_key, w_value, w_out, cache):
    return whole_section(acts[0], norm_gain, final_gain[None], w_query[0], w_key[0], w_value[0], w_out[0], cache[0])


def whole_section(tokens, norm_gain, final_gain, w_query, w_key, w_value, w_out, cache):
    rows, width = tokens.shape
    tensor = lax.axis_size("tensor")
    half = lax.axis_size("segment") // 2
    all_rows = gathered_copies(tokens, "tensor").reshape(tensor * rows, width)
    partial, made = attention(all_rows, norm_gain, w_query, w_key, w_value, w_out, cache)
    segment = lax.axis_index("segment")
    pieces = partial.reshape(tensor, rows, width)
    decoder = segment >= half

    def add_up():
        arrived = lax.all_to_all(pieces, "tensor", 0, 0, tiled=True)
        return residual(arrived, tokens, final_gain)

    new, memory_part = lax.cond(decoder, lambda: (tokens, tokens), add_up)
    firsts = []
    for to in FIRST:
        firsts.append(lax.ppermute(memory_part, "segment", [(half - 1, half + to)]))
    new = lax.cond(decoder, lambda: add_up()[0], lambda: new)
    mine = firsts[0]
    for to, sent in zip(FIRST[1:], firsts[1:]):
        mine = jnp.where(segment == half + to, sent, mine)
    passed = lax.ppermute(mine, "segment", [(half + frm, half + to) for frm, to in SECOND])
    for _, to in SECOND:
        mine = jnp.where(segment == half + to, passed, mine)
    memory = gathered_copies(mine, "tensor").reshape(tensor * rows, width)
    updated, fresh = memory_pair(memory, new, w_key, w_value, made)
    return (updated[None], fresh[None])


def solution(mesh):
    placed = (
        P("segment", ("dp", "tensor"), None),
        P("segment", None),
        P(),
        P("segment", None, "tensor"),
        P("segment", None, "tensor"),
        P("segment", None, "tensor"),
        P("segment", "tensor", None),
        P("segment", None, "dp", "tensor"),
    )
    return jax.shard_map(
        on_device,
        mesh=mesh,
        in_specs=placed,
        out_specs=(P("segment", ("dp", "tensor"), None), P("segment", None, "dp", "tensor")),
        check_vma=False,
    )
```

```python
import jax
import jax.numpy as jnp
from jax import lax
from jax.experimental import pallas as pl
from jax.experimental.pallas import tpu as pltpu
from jax.sharding import PartitionSpec as P

HDIM = 128


EPSILON = 1e-06

SEND_ORDER = (3, 2, 4, 1, 5, 0, 6, 7)


def dot(a, b):
    return jnp.dot(a, b, preferred_element_type=jnp.float32)


def normalize(wide, gain):
    scale = lax.rsqrt(jnp.mean(wide * wide, axis=-1, keepdims=True) + EPSILON)
    return (wide * scale * gain).astype(jnp.bfloat16)


def is_decoder():
    return lax.axis_index("segment") >= lax.axis_size("segment") // 2


def attention_kernel(rows, gain, w_query, w_key, w_value, w_out, cache, partial, made, kv, wk, wv, wo, queries, context, sems):
    decoder = is_decoder()
    encoder = jnp.logical_not(decoder)
    weights = [pltpu.make_async_copy(w_key, wk, sems.at[0]), pltpu.make_async_copy(w_value, wv, sems.at[1])]
    out_copy = pltpu.make_async_copy(w_out, wo, sems.at[2])
    kept = [pltpu.make_async_copy(cache.at[which], kv.at[which], sems.at[3 + which]) for which in range(2)]
    made_copies = [pltpu.make_async_copy(kv.at[which], made.at[which], sems.at[5 + which]) for which in range(2)]

    @pl.when(decoder)
    def _():
        for copy in kept:
            copy.start()

    @pl.when(encoder)
    def _():
        for copy in weights:
            copy.start()

    out_copy.start()
    normed = normalize(rows[...].astype(jnp.float32), gain[...])
    queries[...] = dot(normed, w_query[...]).astype(jnp.bfloat16)

    @pl.when(decoder)
    def _():
        for copy in kept:
            copy.wait()

    @pl.when(encoder)
    def _():
        for which, weight in enumerate((wk, wv)):
            weights[which].wait()
            kv[which] = dot(normed, weight[...]).astype(jnp.bfloat16)
            made_copies[which].start()

    for head in range(queries.shape[1] // HDIM):
        cols = slice(head * HDIM, (head + 1) * HDIM)
        scores = lax.dot_general(queries[:, cols], kv[0, :, cols], (((1,), (1,)), ((), ())), preferred_element_type=jnp.float32)
        weight = jnp.exp(scores - jnp.max(scores, axis=-1, keepdims=True))
        inverse = 1.0 / jnp.sum(weight, axis=-1, keepdims=True)
        context[:, cols] = (dot(weight.astype(jnp.bfloat16), kv[1, :, cols]) * inverse).astype(jnp.bfloat16)
    out_copy.wait()
    partial[...] = dot(context[...], wo[...]).astype(jnp.bfloat16)

    @pl.when(encoder)
    def _():
        for copy in made_copies:
            copy.wait()


NEAR = pl.BlockSpec(memory_space=pltpu.VMEM)
FAR = pl.BlockSpec(memory_space=pltpu.HBM)
PARAMS = pltpu.CompilerParams(vmem_limit_bytes=24 << 20)
EXCHANGE = pl.CostEstimate(flops=20_000_000_000, bytes_accessed=1 << 20, transcendentals=0)


def far(*arrays):
    return [pltpu.with_memory_space_constraint(x, pltpu.HBM) for x in arrays]


def spread_kernel(x, copies, sem):
    copy = pltpu.make_async_copy(x, copies.at[0], sem)
    copy.start()
    copy.wait()
    value = copies[0]
    for to in range(1, copies.shape[0]):
        copies[to] = value


def near_spread_kernel(x, copies):
    for to in range(copies.shape[0]):
        copies[to] = x[...]


def gathered_copies(x, axis, near):
    devices = lax.axis_size(axis)
    copies = pl.pallas_call(
        near_spread_kernel if near else spread_kernel,
        out_shape=jax.ShapeDtypeStruct((devices, *x.shape), x.dtype),
        in_specs=[NEAR if near else FAR],
        out_specs=NEAR,
        scratch_shapes=[] if near else [pltpu.SemaphoreType.DMA],
        compiler_params=PARAMS,
        cost_estimate=EXCHANGE,
        name="spread",
    )(x if near else far(x)[0])
    return lax.all_to_all(copies, axis, 0, 0, tiled=True)


def attention(rows, gain, w_query, w_key, w_value, w_out, cache):
    length, width = rows.shape
    bf16 = jnp.bfloat16
    inner = w_query.shape[1]
    return pl.pallas_call(
        attention_kernel,
        out_shape=(jax.ShapeDtypeStruct((length, width), bf16), jax.ShapeDtypeStruct((2, length, inner), bf16)),
        in_specs=[NEAR] * 3 + [FAR] * 4,
        out_specs=(NEAR, FAR),
        scratch_shapes=[
            pltpu.VMEM((2, length, inner), bf16),
            pltpu.VMEM(w_key.shape, bf16),
            pltpu.VMEM(w_value.shape, bf16),
            pltpu.VMEM(w_out.shape, bf16),
            pltpu.VMEM((length, inner), bf16),
            pltpu.VMEM((length, inner), bf16),
            pltpu.SemaphoreType.DMA((7,)),
        ],
        compiler_params=PARAMS,
        name="section_attention",
    )(rows, gain, w_query, *far(w_key, w_value, w_out, cache))


def residual_kernel(arrived, tokens, gain, updated, memory):
    branch = jnp.sum(arrived[...].astype(jnp.float32), axis=0)
    new = (tokens[...].astype(jnp.float32) + branch).astype(jnp.bfloat16)
    updated[...] = new
    memory[...] = normalize(new.astype(jnp.float32), gain[...])


def residual(arrived, tokens, gain):
    shape = jax.ShapeDtypeStruct(tokens.shape, tokens.dtype)
    return pl.pallas_call(
        residual_kernel,
        out_shape=(shape, shape),
        in_specs=[NEAR, NEAR, NEAR],
        out_specs=(NEAR, NEAR),
        compiler_params=PARAMS,
        name="residual_norm",
    )(arrived, tokens, gain)


def sum_kernel(arrived, tokens, updated):
    branch = jnp.sum(arrived[...].astype(jnp.float32), axis=0)
    updated[...] = (tokens[...].astype(jnp.float32) + branch).astype(jnp.bfloat16)


def residual_only(arrived, tokens):
    return pl.pallas_call(
        sum_kernel,
        out_shape=jax.ShapeDtypeStruct(tokens.shape, tokens.dtype),
        in_specs=[NEAR, NEAR],
        out_specs=NEAR,
        compiler_params=PARAMS,
        name="residual_only",
    )(arrived, tokens)


def memory_kernel(memory, w_key, w_value, fresh, kv, sems):
    pieces = []
    for which, weight in enumerate((w_key, w_value)):
        for part in range(2):
            span = (which, pl.ds(part * (kv.shape[1] // 2), kv.shape[1] // 2))
            copy = pltpu.make_async_copy(kv.at[span], fresh.at[span], sems.at[len(pieces)])
            kv[span] = dot(memory[span[1], :], weight[...]).astype(jnp.bfloat16)
            copy.start()
            pieces.append(copy)
    for copy in pieces:
        copy.wait()


def memory_pair(memory, w_key, w_value):
    shape = (2, memory.shape[0], w_key.shape[1])
    return pl.pallas_call(
        memory_kernel,
        out_shape=jax.ShapeDtypeStruct(shape, memory.dtype),
        in_specs=[NEAR, NEAR, NEAR],
        out_specs=FAR,
        scratch_shapes=[pltpu.VMEM(shape, memory.dtype), pltpu.SemaphoreType.DMA((4,))],
        compiler_params=PARAMS,
        name="memory_pair",
    )(memory, w_key, w_value)


def on_device(acts, norm_gain, final_gain, w_query, w_key, w_value, w_out, cache):
    return whole_section(acts[0], norm_gain, final_gain[None], w_query[0], w_key[0], w_value[0], w_out[0], cache[0])


def whole_section(tokens, norm_gain, final_gain, w_query, w_key, w_value, w_out, cache):
    rows, width = tokens.shape
    tensor = lax.axis_size("tensor")
    half = lax.axis_size("segment") // 2
    all_rows = gathered_copies(tokens, "tensor", False).reshape(tensor * rows, width)
    partial, made = attention(all_rows, norm_gain, w_query, w_key, w_value, w_out, cache)
    segment = lax.axis_index("segment")
    pieces = partial.reshape(tensor, rows, width)
    decoder = segment >= half

    def arrive():
        return lax.all_to_all(pieces, "tensor", 0, 0, tiled=True)

    new, memory_part = lax.cond(decoder, lambda: (tokens, tokens), lambda: residual(arrive(), tokens, final_gain))
    sends = []
    for to in SEND_ORDER:
        sends.append(lax.ppermute(memory_part, "segment", [(half - 1, half + to)]))
    new = lax.cond(decoder, lambda: residual_only(arrive(), tokens), lambda: new)
    mine = sends[0]
    for to, sent in zip(SEND_ORDER[1:], sends[1:]):
        mine = jnp.where(segment == half + to, sent, mine)

    def received():
        memory = gathered_copies(mine, "tensor", True).reshape(tensor * rows, width)
        return memory_pair(memory, w_key, w_value)

    fresh = lax.cond(decoder, received, lambda: made)
    return (new[None], fresh[None])


def solution(mesh):
    placed = (
        P("segment", ("dp", "tensor"), None),
        P("segment", None),
        P(),
        P("segment", None, "tensor"),
        P("segment", None, "tensor"),
        P("segment", None, "tensor"),
        P("segment", "tensor", None),
        P("segment", None, "dp", "tensor"),
    )
    return jax.shard_map(
        on_device,
        mesh=mesh,
        in_specs=placed,
        out_specs=(P("segment", ("dp", "tensor"), None), P("segment", None, "dp", "tensor")),
        check_vma=False,
    )
```

```python
import jax
import jax.numpy as jnp
from jax import lax
from jax.experimental import pallas as pl
from jax.experimental.pallas import tpu as pltpu
from jax.sharding import PartitionSpec as P

HDIM = 128


EPSILON = 1e-06

SEND_ORDER = (3, 2, 4, 1, 5, 0, 6, 7)


def dot(a, b):
    return jnp.dot(a, b, preferred_element_type=jnp.float32)


def normalize(wide, gain):
    scale = lax.rsqrt(jnp.mean(wide * wide, axis=-1, keepdims=True) + EPSILON)
    return (wide * scale * gain).astype(jnp.bfloat16)


def is_decoder():
    return lax.axis_index("segment") >= lax.axis_size("segment") // 2


def attention_kernel(rows, w_query, w_key, w_value, w_out, cache, partial, made, kv, wk, wv, wo, queries, context, sems):
    decoder = is_decoder()
    encoder = jnp.logical_not(decoder)
    weights = [pltpu.make_async_copy(w_key, wk, sems.at[0]), pltpu.make_async_copy(w_value, wv, sems.at[1])]
    out_copy = pltpu.make_async_copy(w_out, wo, sems.at[2])
    kept = [pltpu.make_async_copy(cache.at[which], kv.at[which], sems.at[3 + which]) for which in range(2)]
    made_copies = [pltpu.make_async_copy(kv.at[which], made.at[which], sems.at[5 + which]) for which in range(2)]

    @pl.when(decoder)
    def _():
        for copy in kept:
            copy.start()

    @pl.when(encoder)
    def _():
        for copy in weights:
            copy.start()

    out_copy.start()
    queries[...] = dot(rows[...], w_query[...]).astype(jnp.bfloat16)

    @pl.when(decoder)
    def _():
        for copy in kept:
            copy.wait()

    @pl.when(encoder)
    def _():
        for which, weight in enumerate((wk, wv)):
            weights[which].wait()
            kv[which] = dot(rows[...], weight[...]).astype(jnp.bfloat16)

    for head in range(queries.shape[1] // HDIM):
        cols = slice(head * HDIM, (head + 1) * HDIM)
        scores = lax.dot_general(queries[:, cols], kv[0, :, cols], (((1,), (1,)), ((), ())), preferred_element_type=jnp.float32)
        weight = jnp.exp(scores - jnp.max(scores, axis=-1, keepdims=True))
        inverse = 1.0 / jnp.sum(weight, axis=-1, keepdims=True)
        context[:, cols] = (dot(weight.astype(jnp.bfloat16), kv[1, :, cols]) * inverse).astype(jnp.bfloat16)
    out_copy.wait()

    @pl.when(encoder)
    def _():
        for copy in made_copies:
            copy.start()

    partial[...] = dot(context[...], wo[...]).astype(jnp.bfloat16)

    @pl.when(encoder)
    def _():
        for copy in made_copies:
            copy.wait()


NEAR = pl.BlockSpec(memory_space=pltpu.VMEM)
FAR = pl.BlockSpec(memory_space=pltpu.HBM)
PARAMS = pltpu.CompilerParams(vmem_limit_bytes=24 << 20)
EXCHANGE = pl.CostEstimate(flops=20_000_000_000, bytes_accessed=1 << 20, transcendentals=0)


def far(*arrays):
    return [pltpu.with_memory_space_constraint(x, pltpu.HBM) for x in arrays]


def normed_spread_kernel(x, gain, copies, rows, gains, sems):
    parts = [pltpu.make_async_copy(x, rows, sems.at[0]), pltpu.make_async_copy(gain, gains, sems.at[1])]
    for copy in parts:
        copy.start()
    for copy in parts:
        copy.wait()
    normed = normalize(rows[...].astype(jnp.float32), gains[...])
    for to in range(copies.shape[0]):
        copies[to] = normed


def spread_kernel(x, copies):
    for to in range(copies.shape[0]):
        copies[to] = x[...]


def gathered_copies(x, axis, gain=None):
    devices = lax.axis_size(axis)
    rough = gain is not None
    copies = pl.pallas_call(
        normed_spread_kernel if rough else spread_kernel,
        out_shape=jax.ShapeDtypeStruct((devices, *x.shape), x.dtype),
        in_specs=[FAR, FAR] if rough else [NEAR],
        out_specs=NEAR,
        scratch_shapes=[pltpu.VMEM(x.shape, x.dtype), pltpu.VMEM(gain.shape, gain.dtype), pltpu.SemaphoreType.DMA((2,))] if rough else [],
        compiler_params=PARAMS,
        cost_estimate=EXCHANGE,
        name="spread",
    )(*(far(x, gain) if rough else [x]))
    return lax.all_to_all(copies, axis, 0, 0, tiled=True)


def attention(rows, w_query, w_key, w_value, w_out, cache):
    length, width = rows.shape
    bf16 = jnp.bfloat16
    inner = w_query.shape[1]
    return pl.pallas_call(
        attention_kernel,
        out_shape=(jax.ShapeDtypeStruct((length, width), bf16), jax.ShapeDtypeStruct((2, length, inner), bf16)),
        in_specs=[NEAR] * 2 + [FAR] * 4,
        out_specs=(NEAR, FAR),
        scratch_shapes=[
            pltpu.VMEM((2, length, inner), bf16),
            pltpu.VMEM(w_key.shape, bf16),
            pltpu.VMEM(w_value.shape, bf16),
            pltpu.VMEM(w_out.shape, bf16),
            pltpu.VMEM((length, inner), bf16),
            pltpu.VMEM((length, inner), bf16),
            pltpu.SemaphoreType.DMA((7,)),
        ],
        compiler_params=PARAMS,
        name="section_attention",
    )(rows, w_query, *far(w_key, w_value, w_out, cache))


def residual_kernel(arrived, tokens, gain, updated, memory):
    branch = jnp.sum(arrived[...].astype(jnp.float32), axis=0)
    new = (tokens[...].astype(jnp.float32) + branch).astype(jnp.bfloat16)
    updated[...] = new
    memory[...] = normalize(new.astype(jnp.float32), gain[...])


def residual(arrived, tokens, gain):
    shape = jax.ShapeDtypeStruct(tokens.shape, tokens.dtype)
    return pl.pallas_call(
        residual_kernel,
        out_shape=(shape, shape),
        in_specs=[NEAR, NEAR, NEAR],
        out_specs=(NEAR, NEAR),
        compiler_params=PARAMS,
        name="residual_norm",
    )(arrived, tokens, gain)


def sum_kernel(arrived, tokens, updated):
    branch = jnp.sum(arrived[...].astype(jnp.float32), axis=0)
    updated[...] = (tokens[...].astype(jnp.float32) + branch).astype(jnp.bfloat16)


def residual_only(arrived, tokens):
    return pl.pallas_call(
        sum_kernel,
        out_shape=jax.ShapeDtypeStruct(tokens.shape, tokens.dtype),
        in_specs=[NEAR, NEAR],
        out_specs=NEAR,
        compiler_params=PARAMS,
        name="residual_only",
    )(arrived, tokens)


def memory_kernel(memory, w_key, w_value, fresh, kv, sems):
    pieces = []
    for which, weight in enumerate((w_key, w_value)):
        for part in range(2):
            span = (which, pl.ds(part * (kv.shape[1] // 2), kv.shape[1] // 2))
            copy = pltpu.make_async_copy(kv.at[span], fresh.at[span], sems.at[len(pieces)])
            kv[span] = dot(memory[span[1], :], weight[...]).astype(jnp.bfloat16)
            copy.start()
            pieces.append(copy)
    for copy in pieces:
        copy.wait()


def memory_pair(memory, w_key, w_value):
    shape = (2, memory.shape[0], w_key.shape[1])
    return pl.pallas_call(
        memory_kernel,
        out_shape=jax.ShapeDtypeStruct(shape, memory.dtype),
        in_specs=[NEAR, NEAR, NEAR],
        out_specs=FAR,
        scratch_shapes=[pltpu.VMEM(shape, memory.dtype), pltpu.SemaphoreType.DMA((4,))],
        compiler_params=PARAMS,
        name="memory_pair",
    )(memory, w_key, w_value)


def on_device(acts, norm_gain, final_gain, w_query, w_key, w_value, w_out, cache):
    return whole_section(acts[0], norm_gain, final_gain[None], w_query[0], w_key[0], w_value[0], w_out[0], cache[0])


def whole_section(tokens, norm_gain, final_gain, w_query, w_key, w_value, w_out, cache):
    rows, width = tokens.shape
    tensor = lax.axis_size("tensor")
    half = lax.axis_size("segment") // 2
    all_rows = gathered_copies(tokens, "tensor", norm_gain).reshape(tensor * rows, width)
    partial, made = attention(all_rows, w_query, w_key, w_value, w_out, cache)
    segment = lax.axis_index("segment")
    pieces = partial.reshape(tensor, rows, width)
    decoder = segment >= half

    def arrive():
        return lax.all_to_all(pieces, "tensor", 0, 0, tiled=True)

    new, memory_part = lax.cond(decoder, lambda: (tokens, tokens), lambda: residual(arrive(), tokens, final_gain))
    sends = []
    for to in SEND_ORDER:
        sends.append(lax.ppermute(memory_part, "segment", [(half - 1, half + to)]))
    new = lax.cond(decoder, lambda: residual_only(arrive(), tokens), lambda: new)
    mine = sends[0]
    for to, sent in zip(SEND_ORDER[1:], sends[1:]):
        mine = jnp.where(segment == half + to, sent, mine)

    def received():
        memory = gathered_copies(mine, "tensor").reshape(tensor * rows, width)
        return memory_pair(memory, w_key, w_value)

    fresh = lax.cond(decoder, received, lambda: made)
    return (new[None], fresh[None])


def solution(mesh):
    placed = (
        P("segment", ("dp", "tensor"), None),
        P("segment", None),
        P(),
        P("segment", None, "tensor"),
        P("segment", None, "tensor"),
        P("segment", None, "tensor"),
        P("segment", "tensor", None),
        P("segment", None, "dp", "tensor"),
    )
    return jax.shard_map(
        on_device,
        mesh=mesh,
        in_specs=placed,
        out_specs=(P("segment", ("dp", "tensor"), None), P("segment", None, "dp", "tensor")),
        check_vma=False,
    )
```

```python
import jax
import jax.numpy as jnp
from jax import lax
from jax.experimental import pallas as pl
from jax.experimental.pallas import tpu as pltpu
from jax.sharding import PartitionSpec as P

HDIM = 128


EPSILON = 1e-06

SEND_ORDER = (3, 2, 4, 1, 5, 0, 6, 7)


def dot(a, b):
    return jnp.dot(a, b, preferred_element_type=jnp.float32)


def normalize(wide, gain):
    scale = lax.rsqrt(jnp.mean(wide * wide, axis=-1, keepdims=True) + EPSILON)
    return (wide * scale * gain).astype(jnp.bfloat16)


def is_decoder():
    return lax.axis_index("segment") >= lax.axis_size("segment") // 2


def attention_kernel(rows, w_query, w_key, w_value, w_out, cache, partial, made, kv, wk, wv, wo, queries, context, sems):
    weights = [pltpu.make_async_copy(w_key, wk, sems.at[0]), pltpu.make_async_copy(w_value, wv, sems.at[1])]
    out_copy = pltpu.make_async_copy(w_out, wo, sems.at[2])
    kept = [pltpu.make_async_copy(cache.at[which], kv.at[which], sems.at[3 + which]) for which in range(2)]
    made_copies = [pltpu.make_async_copy(kv.at[which], made.at[which], sems.at[5 + which]) for which in range(2)]

    def section(encoder):
        for copy in weights if encoder else kept:
            copy.start()
        out_copy.start()
        queries[...] = dot(rows[...], w_query[...]).astype(jnp.bfloat16)
        for which, weight in enumerate((wk, wv)):
            if encoder:
                weights[which].wait()
                kv[which] = dot(rows[...], weight[...]).astype(jnp.bfloat16)
            else:
                kept[which].wait()
        for head in range(queries.shape[1] // HDIM):
            cols = slice(head * HDIM, (head + 1) * HDIM)
            scores = lax.dot_general(queries[:, cols], kv[0, :, cols], (((1,), (1,)), ((), ())), preferred_element_type=jnp.float32)
            weight = jnp.exp(scores - jnp.max(scores, axis=-1, keepdims=True))
            inverse = 1.0 / jnp.sum(weight, axis=-1, keepdims=True)
            context[:, cols] = (dot(weight.astype(jnp.bfloat16), kv[1, :, cols]) * inverse).astype(jnp.bfloat16)
        out_copy.wait()
        if encoder:
            for copy in made_copies:
                copy.start()
        partial[...] = dot(context[...], wo[...]).astype(jnp.bfloat16)
        if encoder:
            for copy in made_copies:
                copy.wait()

    decoder = is_decoder()

    @pl.when(decoder)
    def _():
        section(False)

    @pl.when(jnp.logical_not(decoder))
    def _():
        section(True)


NEAR = pl.BlockSpec(memory_space=pltpu.VMEM)
FAR = pl.BlockSpec(memory_space=pltpu.HBM)
PARAMS = pltpu.CompilerParams(vmem_limit_bytes=24 << 20)
EXCHANGE = pl.CostEstimate(flops=20_000_000_000, bytes_accessed=1 << 20, transcendentals=0)


def far(*arrays):
    return [pltpu.with_memory_space_constraint(x, pltpu.HBM) for x in arrays]


def normed_spread_kernel(x, gain, copies, rows, gains, sems):
    parts = [pltpu.make_async_copy(x, rows, sems.at[0]), pltpu.make_async_copy(gain, gains, sems.at[1])]
    for copy in parts:
        copy.start()
    for copy in parts:
        copy.wait()
    normed = normalize(rows[...].astype(jnp.float32), gains[...])
    for to in range(copies.shape[0]):
        copies[to] = normed


def spread_kernel(x, copies):
    for to in range(copies.shape[0]):
        copies[to] = x[...]


def gathered_copies(x, axis, gain=None):
    devices = lax.axis_size(axis)
    rough = gain is not None
    copies = pl.pallas_call(
        normed_spread_kernel if rough else spread_kernel,
        out_shape=jax.ShapeDtypeStruct((devices, *x.shape), x.dtype),
        in_specs=[FAR, FAR] if rough else [NEAR],
        out_specs=NEAR,
        scratch_shapes=[pltpu.VMEM(x.shape, x.dtype), pltpu.VMEM(gain.shape, gain.dtype), pltpu.SemaphoreType.DMA((2,))] if rough else [],
        compiler_params=PARAMS,
        cost_estimate=EXCHANGE,
        name="spread",
    )(*(far(x, gain) if rough else [x]))
    return lax.all_to_all(copies, axis, 0, 0, tiled=True)


def attention(rows, w_query, w_key, w_value, w_out, cache):
    length, width = rows.shape
    bf16 = jnp.bfloat16
    inner = w_query.shape[1]
    return pl.pallas_call(
        attention_kernel,
        out_shape=(jax.ShapeDtypeStruct((length, width), bf16), jax.ShapeDtypeStruct((2, length, inner), bf16)),
        in_specs=[NEAR] * 2 + [FAR] * 4,
        out_specs=(NEAR, FAR),
        scratch_shapes=[
            pltpu.VMEM((2, length, inner), bf16),
            pltpu.VMEM(w_key.shape, bf16),
            pltpu.VMEM(w_value.shape, bf16),
            pltpu.VMEM(w_out.shape, bf16),
            pltpu.VMEM((length, inner), bf16),
            pltpu.VMEM((length, inner), bf16),
            pltpu.SemaphoreType.DMA((7,)),
        ],
        compiler_params=PARAMS,
        name="section_attention",
    )(rows, w_query, *far(w_key, w_value, w_out, cache))


def residual_kernel(arrived, tokens, gain, updated, memory):
    branch = jnp.sum(arrived[...].astype(jnp.float32), axis=0)
    new = (tokens[...].astype(jnp.float32) + branch).astype(jnp.bfloat16)
    updated[...] = new
    memory[...] = normalize(new.astype(jnp.float32), gain[...])


def residual(arrived, tokens, gain):
    shape = jax.ShapeDtypeStruct(tokens.shape, tokens.dtype)
    return pl.pallas_call(
        residual_kernel,
        out_shape=(shape, shape),
        in_specs=[NEAR, NEAR, NEAR],
        out_specs=(NEAR, NEAR),
        compiler_params=PARAMS,
        name="residual_norm",
    )(arrived, tokens, gain)


def sum_kernel(arrived, tokens, updated):
    branch = jnp.sum(arrived[...].astype(jnp.float32), axis=0)
    updated[...] = (tokens[...].astype(jnp.float32) + branch).astype(jnp.bfloat16)


def residual_only(arrived, tokens):
    return pl.pallas_call(
        sum_kernel,
        out_shape=jax.ShapeDtypeStruct(tokens.shape, tokens.dtype),
        in_specs=[NEAR, NEAR],
        out_specs=NEAR,
        compiler_params=PARAMS,
        name="residual_only",
    )(arrived, tokens)


def memory_kernel(memory, w_key, w_value, fresh, kv, sems):
    pieces = []
    for which, weight in enumerate((w_key, w_value)):
        for part in range(2):
            span = (which, pl.ds(part * (kv.shape[1] // 2), kv.shape[1] // 2))
            copy = pltpu.make_async_copy(kv.at[span], fresh.at[span], sems.at[len(pieces)])
            kv[span] = dot(memory[span[1], :], weight[...]).astype(jnp.bfloat16)
            copy.start()
            pieces.append(copy)
    for copy in pieces:
        copy.wait()


def memory_pair(memory, w_key, w_value):
    shape = (2, memory.shape[0], w_key.shape[1])
    return pl.pallas_call(
        memory_kernel,
        out_shape=jax.ShapeDtypeStruct(shape, memory.dtype),
        in_specs=[NEAR, NEAR, NEAR],
        out_specs=FAR,
        scratch_shapes=[pltpu.VMEM(shape, memory.dtype), pltpu.SemaphoreType.DMA((4,))],
        compiler_params=PARAMS,
        name="memory_pair",
    )(memory, w_key, w_value)


def on_device(acts, norm_gain, final_gain, w_query, w_key, w_value, w_out, cache):
    return whole_section(acts[0], norm_gain, final_gain[None], w_query[0], w_key[0], w_value[0], w_out[0], cache[0])


def whole_section(tokens, norm_gain, final_gain, w_query, w_key, w_value, w_out, cache):
    rows, width = tokens.shape
    tensor = lax.axis_size("tensor")
    half = lax.axis_size("segment") // 2
    all_rows = gathered_copies(tokens, "tensor", norm_gain).reshape(tensor * rows, width)
    partial, made = attention(all_rows, w_query, w_key, w_value, w_out, cache)
    segment = lax.axis_index("segment")
    pieces = partial.reshape(tensor, rows, width)
    decoder = segment >= half

    def arrive():
        return lax.all_to_all(pieces, "tensor", 0, 0, tiled=True)

    new, memory_part = lax.cond(decoder, lambda: (tokens, tokens), lambda: residual(arrive(), tokens, final_gain))
    sends = []
    for to in SEND_ORDER:
        sends.append(lax.ppermute(memory_part, "segment", [(half - 1, half + to)]))
    new = lax.cond(decoder, lambda: residual_only(arrive(), tokens), lambda: new)
    mine = sends[0]
    for to, sent in zip(SEND_ORDER[1:], sends[1:]):
        mine = jnp.where(segment == half + to, sent, mine)

    def received():
        memory = gathered_copies(mine, "tensor").reshape(tensor * rows, width)
        return memory_pair(memory, w_key, w_value)

    fresh = lax.cond(decoder, received, lambda: made)
    return (new[None], fresh[None])


def solution(mesh):
    placed = (
        P("segment", ("dp", "tensor"), None),
        P("segment", None),
        P(),
        P("segment", None, "tensor"),
        P("segment", None, "tensor"),
        P("segment", None, "tensor"),
        P("segment", "tensor", None),
        P("segment", None, "dp", "tensor"),
    )
    return jax.shard_map(
        on_device,
        mesh=mesh,
        in_specs=placed,
        out_specs=(P("segment", ("dp", "tensor"), None), P("segment", None, "dp", "tensor")),
        check_vma=False,
    )
```
